768 devices in a mesh: grp: 8 (over y_hi, core), row: 24 (over y_lo, z), col: 4 (over x).
Axes of the slice: x: 4, y: 8 (y_hi: 4, y_lo: 2; y = y_hi * 2 + y_lo), z: 12, core: 2. Of those that a mesh axis runs over, the one named last changes fastest.
Arguments:
- field: float32 [8, 8, 3072, 1536], P(None, 'grp', 'row', 'col'), may hold values from -6 to 6
- previous: bfloat16 [8, 8, 3072, 1536], P(None, 'grp', 'row', 'col'), may hold values from -6 to 6
- kappa: float32 [8, 3072, 1536], P('grp', 'row', 'col'), may hold values from 0.02 to 0.1
- rates: float32 [8], replicated, may hold values from 0.5 to 1.6
- speeds: float32 [8, 3], replicated, may hold values from -0.5 to 0.5
- basis_x: bfloat16 [3072, 128], replicated, may hold values from -0.109375 to 0.109375
- basis_y: bfloat16 [1536, 128], replicated, may hold values from -0.15625 to 0.15625
Outputs:
- advanced: float32 [8, 8, 3072, 1536], P(None, 'grp', 'row', 'col')
- core: float32 [8, 8, 128, 128], P(None, 'grp')
- gram_x: float32 [3072, 128], P('row')
- gram_y: float32 [1536, 128], P(('col', 'row'))
The draws below stay inside these ranges and needn't reach their ends.
All inputs are finite; a program needn't handle non-finite values.
Results may differ from the reference program's by a relative error of at most 0.0029.
Values may be sent and summed in bfloat16 or wider, within the bound.
No kernel may reach another device: no remote copies, remote signals or barrier semaphores. Data moves between devices by JAX's collectives and lax.ppermute only.
A program may use at most 64 MiB of HBM per device.

```python
import math
import jax
import jax.numpy as jnp
from jax import lax

SPECIES = 8
RANK = 128
NX = 3072
NY = 1536
NZ = 8


def levels(rng, dims, cuts, low, largest):
    gain = 1.0
    for position, shards_of in cuts:
        steps = jax.random.uniform(jax.random.fold_in(jax.random.fold_in(rng, 6), position), (shards_of,), jnp.float32, low / len(cuts), largest / len(cuts))
        gain = gain * jnp.repeat(jnp.exp(steps), dims[position] // shards_of).reshape((-1,) + (1,) * (len(dims) - 1 - position))
    return gain


def gaussian(rng, shape, scale, bound, pieces=(), kind=jnp.bfloat16):
    array = jax.random.normal(rng, shape, jnp.float32) * scale
    if len(pieces) > 0:
        array = levels(rng, shape, pieces, -0.22, 0.18) * array
    return jnp.clip(array, min=-bound, max=bound).astype(kind)


def setup_inputs(seed: int = 0) -> dict:
    splits = jax.random.split(jax.random.key(seed), 8)
    return {
        "field": gaussian(splits[0], (SPECIES, NZ, NX, NY), 1.0, 6.0, ((1, 8), (2, 24), (3, 4)), jnp.float32),
        "previous": gaussian(splits[1], (SPECIES, NZ, NX, NY), 1.0, 6.0, ((1, 8), (2, 24), (3, 4))),
        "kappa": jnp.clip(jnp.exp(math.log(0.1) - 1.609438 * jax.random.uniform(splits[2], (NZ, NX, NY), jnp.float32) ** levels(splits[2], (NZ, NX, NY), ((0, 8), (1, 24), (2, 4)), -0.2, 0.2)), 0.02, 0.1),
        "rates": jnp.clip(jnp.exp(jax.random.uniform(splits[3], (SPECIES,), jnp.float32, math.log(0.5), math.log(1.6))), 0.5, 1.6),
        "speeds": jnp.clip(jax.random.uniform(splits[4], (SPECIES, 3), jnp.float32, -0.5, 0.5), -0.5, 0.5),
        "basis_x": gaussian(splits[5], (NX, RANK), NX ** -0.5, 0.109375),
        "basis_y": gaussian(splits[6], (NY, RANK), NY ** -0.5, 0.15625),
    }


def advance_species(packed):
    values, rate, speed, kappa = packed
    padded = jnp.pad(values, 1)
    z_next = padded[2:, 1:-1, 1:-1]
    z_prev = padded[:-2, 1:-1, 1:-1]
    x_next = padded[1:-1, 2:, 1:-1]
    x_prev = padded[1:-1, :-2, 1:-1]
    y_next = padded[1:-1, 1:-1, 2:]
    y_prev = padded[1:-1, 1:-1, :-2]
    laplace = z_next + z_prev + x_next + x_prev + y_next + y_prev - 6.0 * values
    transport = speed[0] * (z_next - z_prev) + speed[1] * (x_next - x_prev) + speed[2] * (y_next - y_prev)
    return values + kappa * rate * laplace - 0.5 * transport

def reference(field, previous, kappa, rates, speeds, basis_x, basis_y):
    high = lax.Precision.HIGHEST
    advanced = lax.map(lambda item: advance_species((item[0], item[1], item[2], kappa)), (field, rates, speeds))
    wide_x = basis_x.astype(jnp.float32)

    def project_species(slab):
        slab_wide = slab.astype(jnp.float32)
        projected = jnp.einsum('zxy,xr->zyr', slab_wide, wide_x, precision=high).astype(jnp.bfloat16)
        partial_x = jnp.einsum('zxy,zyr->xr', slab_wide, projected.astype(jnp.float32), precision=high)
        return (projected, partial_x)
    projected, partials = lax.map(project_species, previous)
    proj_wide = projected.astype(jnp.float32)
    core = jnp.einsum('szyr,yq->szrq', proj_wide, basis_y.astype(jnp.float32), precision=high)
    core_low = core.astype(jnp.bfloat16).astype(jnp.float32)
    scale_y = math.sqrt(NY) / (SPECIES * NZ * RANK)
    gram_y = scale_y * jnp.einsum('szyr,szrq->yq', proj_wide, core_low, precision=high)
    scale_x = math.sqrt(NX) / (SPECIES * NZ * NY)
    gram_x = scale_x * lax.optimization_barrier(jnp.sum(partials, axis=0))
    return (advanced, core, gram_x, gram_y)
```

```python
import math

import jax
import jax.numpy as jnp
from jax import lax
from jax.sharding import Mesh
from jax.sharding import PartitionSpec as P

F32 = jnp.float32
BF16 = jnp.bfloat16
GRP = ("yh", "core")
ROW = ("yl", "zh", "zl")
QUAD = ("yl", "zl")


def chain(n):
    return [(i, i + 1) for i in range(n - 1)]


def back(n):
    return [(i + 1, i) for i in range(n - 1)]


def exchanged(value, axes):
    return lax.all_to_all(value, axes, 0, 0, tiled=True)


def dot(a, b, dims):
    return lax.dot_general(a, b, dims, preferred_element_type=F32)


def stencil(field, kappa, rates, speeds):
    u = field[:, 0]
    n_grp, n_row, n_col = lax.axis_size(GRP), lax.axis_size(ROW), lax.axis_size("x")
    low = u.astype(BF16)
    z_prev = lax.ppermute(low, GRP, chain(n_grp)).astype(F32)
    z_next = lax.ppermute(low, GRP, back(n_grp)).astype(F32)
    x_low = lax.ppermute(u[:, -1, :], ROW, chain(n_row))
    x_high = lax.ppermute(u[:, 0, :], ROW, back(n_row))
    y_low = lax.ppermute(u[:, :, -1], "x", chain(n_col))
    y_high = lax.ppermute(u[:, :, 0], "x", back(n_col))
    x_prev = jnp.concatenate([x_low[:, None, :], u[:, :-1, :]], axis=1)
    x_next = jnp.concatenate([u[:, 1:, :], x_high[:, None, :]], axis=1)
    y_prev = jnp.concatenate([y_low[:, :, None], u[:, :, :-1]], axis=2)
    y_next = jnp.concatenate([u[:, :, 1:], y_high[:, :, None]], axis=2)
    laplace = z_next + z_prev + x_next + x_prev + y_next + y_prev - 6.0 * u
    sz, sx, sy = (speeds[:, d][:, None, None] for d in range(3))
    transport = sz * (z_next - z_prev) + sx * (x_next - x_prev) + sy * (y_next - y_prev)
    out = u + kappa * rates[:, None, None] * laplace - 0.5 * transport
    return out[:, None]


def on_device(field, previous, kappa, rates, speeds, basis_x, basis_y):
    species, depth, width_x, width_y = field.shape
    rank = basis_x.shape[1]
    n_quad, n_zh, n_col = lax.axis_size(QUAD), lax.axis_size("zh"), lax.axis_size("x")
    n_grp, n_row = lax.axis_size(GRP), lax.axis_size(ROW)
    own = species // n_quad
    grid_x, grid_y, grid_z = width_x * n_row, width_y * n_col, depth * n_grp
    part_y = width_y // n_row
    scale_x = math.sqrt(grid_x) / (species * grid_z * grid_y)
    scale_y = math.sqrt(grid_y) / (species * grid_z * rank)
    zh = lax.axis_index("zh")

    advanced = stencil(field, kappa, rates, speeds)

    lines = exchanged(previous.reshape(n_quad, own, width_x, width_y), QUAD)
    bx = basis_x.reshape(lax.axis_size("yl"), n_zh, lax.axis_size("zl"), width_x, rank)
    bx = lax.dynamic_index_in_dim(bx, zh, 1, keepdims=False).reshape(n_quad, width_x, rank)
    partial = sum(
        dot(lines[j], bx[j], (((1,), (0,)), ((), ()))) for j in range(n_quad)
    )
    pieces = partial.reshape(n_zh, own * width_y // n_zh, rank)
    mine = exchanged(pieces, "zh").sum(axis=0).astype(BF16)
    projected = lax.all_gather(mine, "zh", tiled=True).reshape(own, width_y, rank)

    by = lax.dynamic_slice_in_dim(basis_y, lax.axis_index("x") * width_y, width_y, 0)
    core_part = dot(projected, by, (((1,), (0,)), ((), ())))
    core_own = lax.all_gather(core_part, "x").sum(axis=0)
    core = lax.all_gather(core_own, QUAD, tiled=True)[:, None]

    gx = jnp.stack(
        [
            sum(
                dot(lines[j, s], projected[s], (((1,), (0,)), ((), ())))
                for s in range(own)
            )
            for j in range(n_quad)
        ]
    )
    gx = exchanged(scale_x * gx, QUAD).sum(axis=0)
    gx = lax.all_gather(gx, "x").sum(axis=0)
    gram_x = lax.all_gather(gx, GRP).sum(axis=0)

    half = part_y * lax.axis_size("zl")
    rows = projected.reshape(own, lax.axis_size("yl"), n_zh, half, rank)
    rows = lax.dynamic_index_in_dim(rows, zh, 2, keepdims=False)
    rows = rows.reshape(own, n_quad * part_y, rank)
    core_low = core_own.astype(BF16)
    gy = scale_y * sum(dot(rows[s], core_low[s], (((1,), (0,)), ((), ()))) for s in range(own))
    gy = exchanged(gy.reshape(n_quad, part_y, rank), QUAD).sum(axis=0)
    gram_y = lax.all_gather(gy, GRP).sum(axis=0)
    return (advanced, core, gram_x, gram_y)


def solution(mesh):
    split = Mesh(
        mesh.devices.reshape(4, 2, 2, 6, 2, 4), ("yh", "core", "yl", "zh", "zl", "x")
    )
    block = P(None, GRP, ROW, "x")
    return jax.shard_map(
        on_device,
        mesh=split,
        in_specs=(block, block, P(GRP, ROW, "x"), P(), P(), P(), P()),
        out_specs=(block, P(None, GRP, None, None), P(ROW, None), P(("x", *ROW), None)),
        check_vma=False,
    )
```

```python
import functools
import math

import jax
import jax.numpy as jnp
from jax import lax
from jax.experimental import pallas as pl
from jax.experimental.pallas import tpu as pltpu
from jax.sharding import Mesh
from jax.sharding import PartitionSpec as P


F32 = jnp.float32
BF16 = jnp.bfloat16
GRP = ("yh", "core")
ROW = ("yl", "zh", "zl")
QUAD = ("yl", "zl")
LANES = 128
WHOLE = pl.BlockSpec(memory_space=pltpu.VMEM)
SCALARS = pl.BlockSpec(memory_space=pltpu.SMEM)


def call(kernel, **given):
    def run(*args):
        return pl.pallas_call(kernel, **given)(*args)

    return run


def chain(n):
    return [(i, i + 1) for i in range(n - 1)]


def back(n):
    return [(i + 1, i) for i in range(n - 1)]


def exchanged(value, axes):
    return lax.all_to_all(value, axes, 0, 0, tiled=True)


def shape(dims, kind):
    return jax.ShapeDtypeStruct(dims, kind)


def dot_t(a, b):
    return lax.dot_general(a, b, (((0,), (0,)), ((), ())), preferred_element_type=F32)


def dot(a, b):
    return lax.dot_general(a, b, (((1,), (0,)), ((), ())), preferred_element_type=F32)


GRANT = pltpu.CompilerParams(vmem_limit_bytes=16 * 2**20)


def cost(flops):
    return pl.CostEstimate(flops=flops, bytes_accessed=1 << 20, transcendentals=0)


def faces_kernel(u_ref, low_ref, x_first, x_last, y_first, y_last):
    u = u_ref[0]
    low = u.astype(BF16)
    low_ref[0] = low
    x_first[0] = u[:1]
    x_last[0] = u[-1:]
    y_first[0] = low[:, :LANES]
    y_last[0] = low[:, -LANES:]


def faces(u):
    species, wx, wy = u.shape
    plane = pl.BlockSpec((1, wx, wy), lambda s: (s, 0, 0))
    line = pl.BlockSpec((1, 1, wy), lambda s: (s, 0, 0))
    strip = pl.BlockSpec((1, wx, LANES), lambda s: (s, 0, 0))
    return call(
        faces_kernel,
        grid=(species,),
        in_specs=[plane],
        out_specs=[plane, line, line, strip, strip],
        out_shape=[
            shape(u.shape, BF16),
            shape((species, 1, wy), F32),
            shape((species, 1, wy), F32),
            shape((species, wx, LANES), BF16),
            shape((species, wx, LANES), BF16),
        ],
        cost_estimate=cost(10**8),
        compiler_params=GRANT,
    )(u)


def stencil_kernel(rates, speeds, u_ref, zp, zn, xp, xn, yp, yn, kappa, out):
    s = pl.program_id(0)
    u = u_ref[0]
    wx, wy = u.shape
    rows = lax.broadcasted_iota(jnp.int32, u.shape, 0)
    lanes = lax.broadcasted_iota(jnp.int32, u.shape, 1)
    z_prev, z_next = zp[0].astype(F32), zn[0].astype(F32)
    x_prev = jnp.where(rows == 0, xp[0], pltpu.roll(u, 1, 0))
    x_next = jnp.where(rows == wx - 1, xn[0], pltpu.roll(u, wx - 1, 0))
    y_prev = jnp.where(lanes == 0, yp[0].astype(F32)[:, -1:], pltpu.roll(u, 1, 1))
    y_next = jnp.where(lanes == wy - 1, yn[0].astype(F32)[:, :1], pltpu.roll(u, wy - 1, 1))
    laplace = z_next + z_prev + x_next + x_prev + y_next + y_prev - 6.0 * u
    transport = (
        speeds[s, 0] * (z_next - z_prev)
        + speeds[s, 1] * (x_next - x_prev)
        + speeds[s, 2] * (y_next - y_prev)
    )
    out[0] = u + kappa[...] * rates[s] * laplace - 0.5 * transport


def stencil(u, kappa, rates, speeds):
    species, wx, wy = u.shape
    n_grp, n_row, n_col = lax.axis_size(GRP), lax.axis_size(ROW), lax.axis_size("x")
    low, x_first, x_last, y_first, y_last = faces(u)
    z_prev = lax.ppermute(low, GRP, chain(n_grp))
    z_next = lax.ppermute(low, GRP, back(n_grp))
    x_prev = lax.ppermute(x_last, ROW, chain(n_row))
    x_next = lax.ppermute(x_first, ROW, back(n_row))
    y_prev = lax.ppermute(y_last, "x", chain(n_col))
    y_next = lax.ppermute(y_first, "x", back(n_col))
    plane = pl.BlockSpec((1, wx, wy), lambda s: (s, 0, 0))
    line = pl.BlockSpec((1, 1, wy), lambda s: (s, 0, 0))
    strip = pl.BlockSpec((1, wx, LANES), lambda s: (s, 0, 0))
    return call(
        stencil_kernel,
        grid=(species,),
        in_specs=[SCALARS, SCALARS, plane, plane, plane, line, line, strip, strip]
        + [pl.BlockSpec((wx, wy), lambda s: (0, 0))],
        out_specs=plane,
        out_shape=shape(u.shape, F32),
        cost_estimate=cost(10**9),
        compiler_params=GRANT,
    )(rates, speeds, u, z_prev, z_next, x_prev, x_next, y_prev, y_next, kappa)


def project_kernel(lines, basis, out):
    quad, own, wx, wy = lines.shape
    rank = basis.shape[-1]
    b = basis[...].reshape(quad * wx, rank)
    for s in range(own):
        block = lines[:, s].reshape(quad * wx, wy)
        out[s] = dot_t(block, b)


def round_kernel(parts, out):
    total = parts[0]
    for k in range(1, parts.shape[0]):
        total = total + parts[k]
    low = total.astype(BF16)
    for k in range(out.shape[0]):
        out[k] = low


def moments_kernel(scale, lines, projected, basis, out):
    quad, own, wx, wy = lines.shape
    rank = projected.shape[-1]
    columns, part = out.shape[0], wx // out.shape[0]
    for s in range(own):
        core = dot_t(projected[s], basis[...])
        high = core.astype(BF16)
        low = (core - high.astype(F32)).astype(BF16)
        for k in range(columns):
            out[k, pl.ds(s * rank, rank)] = high
            out[k, pl.ds((own + s) * rank, rank)] = low
    total = dot(lines[:, 0].reshape(quad * wx, wy), projected[0])
    for s in range(1, own):
        total = total + dot(lines[:, s].reshape(quad * wx, wy), projected[s])
    total = (scale * total).astype(BF16)
    first = 2 * own * rank
    for q in range(quad):
        for k in range(columns):
            rows = total[q * wx + k * part : q * wx + (k + 1) * part]
            out[k, pl.ds(first + q * part, part)] = rows


def mix_kernel(scale, zh, parts, projected, out):
    own, wy, rank = projected.shape
    columns, quad = parts.shape[0], out.shape[0]
    part = (parts.shape[1] - 2 * own * rank) // quad
    half_rows = 2 * (out.shape[1] - own * rank - part)
    totals = [0.0, 0.0]
    for s in range(own):
        total = 0.0
        for first in (s * rank, (own + s) * rank):
            for k in range(columns):
                total = total + parts[k, pl.ds(first, rank)].astype(F32)
        low = total.astype(BF16)
        for q in range(quad):
            out[q, pl.ds(s * rank, rank)] = low
        for h in range(2):
            first = pl.multiple_of(h * (wy // 2) + zh[0] * half_rows, half_rows)
            totals[h] = totals[h] + dot(projected[s, pl.ds(first, half_rows), :], low)
    for q in range(quad):
        total = 0.0
        for k in range(columns):
            total = total + parts[k, pl.ds(2 * own * rank + q * part, part)].astype(F32)
        out[q, pl.ds(own * rank, part)] = total.astype(BF16)
    for h in range(2):
        rows = (scale * totals[h]).astype(BF16)
        for low in range(2):
            size = half_rows // 2
            out[2 * h + low, pl.ds(own * rank + part, size)] = rows[low * size : (low + 1) * size]


def spread_kernel(parts, core, out):
    quad, n = parts.shape[0], core.shape[1]
    total = 0.0
    for q in range(quad):
        core[q] = parts[q, :n].astype(F32)
        total = total + parts[q, n:].astype(F32)
    low = total.astype(BF16)
    for k in range(out.shape[0]):
        out[k] = low


def last_kernel(column, parts, gram_x, gram_y):
    groups, columns = parts.shape[:2]
    part = gram_x.shape[0] // columns
    for c in range(columns):
        total = parts[0, c, :part].astype(F32)
        for g in range(1, groups):
            total = total + parts[g, c, :part].astype(F32)
        gram_x[pl.ds(c * part, part)] = total
    mine = column[0]
    total = parts[0, mine, part:].astype(F32)
    for g in range(1, groups):
        total = total + parts[g, mine, part:].astype(F32)
    gram_y[...] = total


def on_device(field, previous, kappa, rates, speeds, basis_x, basis_y):
    species, depth, width_x, width_y = field.shape
    rank = basis_x.shape[1]
    n_quad, n_zh, n_col = lax.axis_size(QUAD), lax.axis_size("zh"), lax.axis_size("x")
    n_grp, n_row = lax.axis_size(GRP), lax.axis_size(ROW)
    own = species // n_quad
    grid_x, grid_y, grid_z = width_x * n_row, width_y * n_col, depth * n_grp
    part_y = width_y // n_row
    scale_x = math.sqrt(grid_x) / (species * grid_z * grid_y)
    scale_y = math.sqrt(grid_y) / (species * grid_z * rank)
    zh = lax.axis_index("zh")

    lines = exchanged(previous.reshape(n_quad, own, width_x, width_y), QUAD)
    bx = basis_x.reshape(lax.axis_size("yl"), n_zh, lax.axis_size("zl"), width_x, rank)
    bx = lax.dynamic_index_in_dim(bx, zh, 1, keepdims=False).reshape(n_quad, width_x, rank)
    by = lax.dynamic_slice_in_dim(basis_y, lax.axis_index("x") * width_y, width_y, 0)
    advanced = stencil(field[:, 0], kappa[0], rates, speeds)[:, None]

    partial = call(
        project_kernel,
        in_specs=[WHOLE, WHOLE],
        out_specs=WHOLE,
        out_shape=shape((own, width_y, rank), F32),
        cost_estimate=cost(2 * n_quad * width_x * own * width_y * rank),
        compiler_params=GRANT,
    )(lines, bx)
    piece = own * width_y // n_zh
    arrived = exchanged(partial.reshape(n_zh, piece, rank), "zh")
    mine = call(
        round_kernel,
        in_specs=[WHOLE],
        out_specs=WHOLE,
        out_shape=shape((n_zh, piece, rank), BF16),
        cost_estimate=cost(10**7),
        compiler_params=GRANT,
    )(arrived)
    projected = exchanged(mine, "zh").reshape(own, width_y, rank)

    part_x = width_x // n_col
    moments = call(
        functools.partial(moments_kernel, scale_x),
        in_specs=[WHOLE, WHOLE, WHOLE],
        out_specs=WHOLE,
        out_shape=shape((n_col, 2 * own * rank + n_quad * part_x, rank), BF16),
        cost_estimate=cost(4 * n_quad * width_x * own * width_y * rank),
        compiler_params=GRANT,
    )(lines, projected, by)
    mixed = call(
        functools.partial(mix_kernel, scale_y),
        in_specs=[SCALARS, WHOLE, WHOLE],
        out_specs=WHOLE,
        out_shape=shape((n_quad, own * rank + part_x + part_y, rank), BF16),
        cost_estimate=cost(10**8),
        compiler_params=GRANT,
    )(zh.reshape(1), exchanged(moments, "x"), projected)
    core, rows = call(
        spread_kernel,
        in_specs=[WHOLE],
        out_specs=[WHOLE, WHOLE],
        out_shape=[
            shape((n_quad, own * rank, rank), F32),
            shape((n_grp * n_col, part_x + part_y, rank), BF16),
        ],
        cost_estimate=cost(10**8),
        compiler_params=GRANT,
    )(exchanged(mixed, QUAD))
    core = core.reshape(species, 1, rank, rank)
    rows = exchanged(rows, GRP + ("x",))
    gram_x, gram_y = call(
        last_kernel,
        in_specs=[SCALARS, WHOLE],
        out_specs=[WHOLE, WHOLE],
        out_shape=[shape((width_x, rank), F32), shape((part_y, rank), F32)],
        cost_estimate=cost(10**7),
        compiler_params=GRANT,
    )(lax.axis_index("x").reshape(1), rows.reshape(n_grp, n_col, part_x + part_y, rank))
    return (advanced, core, gram_x, gram_y)


def solution(mesh):
    split = Mesh(
        mesh.devices.reshape(4, 2, 2, 6, 2, 4), ("yh", "core", "yl", "zh", "zl", "x")
    )
    block = P(None, GRP, ROW, "x")
    return jax.shard_map(
        on_device,
        mesh=split,
        in_specs=(block, block, P(GRP, ROW, "x"), P(), P(), P(), P()),
        out_specs=(block, P(None, GRP, None, None), P(ROW, None), P(("x", *ROW), None)),
        check_vma=False,
    )
```

```python
import functools
import math

import jax
import jax.numpy as jnp
from jax import lax
from jax.experimental import pallas as pl
from jax.experimental.pallas import tpu as pltpu
from jax.sharding import Mesh
from jax.sharding import PartitionSpec as P


F32 = jnp.float32
BF16 = jnp.bfloat16
GRP = ("yh", "core")
ROW = ("yl", "zh", "zl")
QUAD = ("yl", "zl")
LANES = 128
WHOLE = pl.BlockSpec(memory_space=pltpu.VMEM)
SCALARS = pl.BlockSpec(memory_space=pltpu.SMEM)


def call(kernel, **given):
    def run(*args):
        return pl.pallas_call(kernel, **given)(*args)

    return run


def chain(n):
    return [(i, i + 1) for i in range(n - 1)]


def back(n):
    return [(i + 1, i) for i in range(n - 1)]


def exchanged(value, axes):
    return lax.all_to_all(value, axes, 0, 0, tiled=True)


def stored(dims, kind):
    return pltpu.HBM(dims, kind)


def shape(dims, kind):
    return jax.ShapeDtypeStruct(dims, kind)


def dot_t(a, b):
    return lax.dot_general(a, b, (((0,), (0,)), ((), ())), preferred_element_type=F32)


def dot(a, b):
    return lax.dot_general(a, b, (((1,), (0,)), ((), ())), preferred_element_type=F32)


GRANT = pltpu.CompilerParams(vmem_limit_bytes=16 * 2**20)


def cost(flops):
    return pl.CostEstimate(flops=flops, bytes_accessed=1 << 20, transcendentals=0)


def faces_kernel(u_ref, low_ref, x_first, x_last, y_first, y_last):
    u = u_ref[0]
    low = u.astype(BF16)
    low_ref[0] = low
    x_first[0] = u[:1]
    x_last[0] = u[-1:]
    y_first[0] = low[:, :LANES]
    y_last[0] = low[:, -LANES:]


def faces(u):
    species, wx, wy = u.shape
    plane = pl.BlockSpec((1, wx, wy), lambda s: (s, 0, 0))
    line = pl.BlockSpec((1, 1, wy), lambda s: (s, 0, 0))
    strip = pl.BlockSpec((1, wx, LANES), lambda s: (s, 0, 0))
    return call(
        faces_kernel,
        grid=(species,),
        in_specs=[plane],
        out_specs=[plane, line, line, strip, strip],
        out_shape=[
            stored(u.shape, BF16),
            stored((species, 1, wy), F32),
            stored((species, 1, wy), F32),
            stored((species, wx, LANES), BF16),
            stored((species, wx, LANES), BF16),
        ],
        cost_estimate=cost(10**8),
        compiler_params=GRANT,
    )(u)


def stencil_kernel(rates, speeds, u_ref, zp, zn, xp, xn, yp, yn, kappa, out):
    s = pl.program_id(0)
    u = u_ref[0]
    wx, wy = u.shape
    rows = lax.broadcasted_iota(jnp.int32, u.shape, 0)
    lanes = lax.broadcasted_iota(jnp.int32, u.shape, 1)
    z_prev, z_next = zp[0].astype(F32), zn[0].astype(F32)
    x_prev = jnp.where(rows == 0, xp[0], pltpu.roll(u, 1, 0))
    x_next = jnp.where(rows == wx - 1, xn[0], pltpu.roll(u, wx - 1, 0))
    y_prev = jnp.where(lanes == 0, yp[0].astype(F32)[:, -1:], pltpu.roll(u, 1, 1))
    y_next = jnp.where(lanes == wy - 1, yn[0].astype(F32)[:, :1], pltpu.roll(u, wy - 1, 1))
    laplace = z_next + z_prev + x_next + x_prev + y_next + y_prev - 6.0 * u
    transport = (
        speeds[s, 0] * (z_next - z_prev)
        + speeds[s, 1] * (x_next - x_prev)
        + speeds[s, 2] * (y_next - y_prev)
    )
    out[0] = u + kappa[...] * rates[s] * laplace - 0.5 * transport


def stencil(u, kappa, rates, speeds):
    species, wx, wy = u.shape
    n_grp, n_row, n_col = lax.axis_size(GRP), lax.axis_size(ROW), lax.axis_size("x")
    low, x_first, x_last, y_first, y_last = faces(u)
    z_prev = lax.ppermute(low, GRP, chain(n_grp))
    z_next = lax.ppermute(low, GRP, back(n_grp))
    x_prev = lax.ppermute(x_last, ROW, chain(n_row))
    x_next = lax.ppermute(x_first, ROW, back(n_row))
    y_prev = lax.ppermute(y_last, "x", chain(n_col))
    y_next = lax.ppermute(y_first, "x", back(n_col))
    plane = pl.BlockSpec((1, wx, wy), lambda s: (s, 0, 0))
    line = pl.BlockSpec((1, 1, wy), lambda s: (s, 0, 0))
    strip = pl.BlockSpec((1, wx, LANES), lambda s: (s, 0, 0))
    return call(
        stencil_kernel,
        grid=(species,),
        in_specs=[SCALARS, SCALARS, plane, plane, plane, line, line, strip, strip]
        + [pl.BlockSpec((wx, wy), lambda s: (0, 0))],
        out_specs=plane,
        out_shape=shape(u.shape, F32),
        cost_estimate=cost(10**9),
        compiler_params=GRANT,
    )(rates, speeds, u, z_prev, z_next, x_prev, x_next, y_prev, y_next, kappa)


def project_kernel(lines, basis, out):
    quad, own, wx, wy = lines.shape
    rank = basis.shape[-1]
    b = basis[...].reshape(quad * wx, rank)
    for s in range(own):
        block = lines[:, s].reshape(quad * wx, wy)
        out[s] = dot_t(block, b)


def round_kernel(parts, out):
    total = parts[0]
    for k in range(1, parts.shape[0]):
        total = total + parts[k]
    low = total.astype(BF16)
    for k in range(out.shape[0]):
        out[k] = low


def moments_kernel(scale, lines, projected, basis, out):
    quad, own, wx, wy = lines.shape
    rank = projected.shape[-1]
    columns = out.shape[0]
    for s in range(own):
        core = dot_t(projected[s], basis[...])
        high = core.astype(BF16)
        low = (core - high.astype(F32)).astype(BF16)
        for k in range(columns):
            out[k, pl.ds(s * rank, rank)] = high
            out[k, pl.ds((own + s) * rank, rank)] = low
    total = dot(lines[:, 0].reshape(quad * wx, wy), projected[0])
    for s in range(1, own):
        total = total + dot(lines[:, s].reshape(quad * wx, wy), projected[s])
    total = (scale * total).astype(BF16)
    for k in range(columns):
        out[k, pl.ds(2 * own * rank, quad * wx)] = total


def mix_kernel(scale, zh, parts, projected, out):
    own, wy, rank = projected.shape
    columns, quad = parts.shape[0], out.shape[0]
    part = (parts.shape[1] - 2 * own * rank) // quad
    half_rows = 2 * (out.shape[1] - own * rank - part)
    totals = [0.0, 0.0]
    for s in range(own):
        total = 0.0
        for first in (s * rank, (own + s) * rank):
            for k in range(columns):
                total = total + parts[k, pl.ds(first, rank)].astype(F32)
        low = total.astype(BF16)
        for q in range(quad):
            out[q, pl.ds(s * rank, rank)] = low
        for h in range(2):
            first = pl.multiple_of(h * (wy // 2) + zh[0] * half_rows, half_rows)
            totals[h] = totals[h] + dot(projected[s, pl.ds(first, half_rows), :], low)
    for q in range(quad):
        total = 0.0
        for k in range(columns):
            total = total + parts[k, pl.ds(2 * own * rank + q * part, part)].astype(F32)
        out[q, pl.ds(own * rank, part)] = total.astype(BF16)
    for h in range(2):
        rows = (scale * totals[h]).astype(BF16)
        for low in range(2):
            size = half_rows // 2
            out[2 * h + low, pl.ds(own * rank + part, size)] = rows[low * size : (low + 1) * size]


def spread_kernel(parts, core, out):
    quad, n = parts.shape[0], core.shape[1]
    total = 0.0
    for q in range(quad):
        core[q] = parts[q, :n].astype(F32)
        total = total + parts[q, n:].astype(F32)
    low = total.astype(BF16)
    for k in range(out.shape[0]):
        out[k] = low


def last_kernel(parts, gram_x, gram_y):
    total = parts[0].astype(F32)
    for g in range(1, parts.shape[0]):
        total = total + parts[g].astype(F32)
    n = gram_x.shape[0]
    gram_x[...] = total[:n]
    gram_y[...] = total[n:]


def on_device(field, previous, kappa, rates, speeds, basis_x, basis_y):
    species, depth, width_x, width_y = field.shape
    rank = basis_x.shape[1]
    n_quad, n_zh, n_col = lax.axis_size(QUAD), lax.axis_size("zh"), lax.axis_size("x")
    n_grp, n_row = lax.axis_size(GRP), lax.axis_size(ROW)
    own = species // n_quad
    grid_x, grid_y, grid_z = width_x * n_row, width_y * n_col, depth * n_grp
    part_y = width_y // n_row
    scale_x = math.sqrt(grid_x) / (species * grid_z * grid_y)
    scale_y = math.sqrt(grid_y) / (species * grid_z * rank)
    zh = lax.axis_index("zh")

    lines = exchanged(previous.reshape(n_quad, own, width_x, width_y), QUAD)
    bx = basis_x.reshape(lax.axis_size("yl"), n_zh, lax.axis_size("zl"), width_x, rank)
    bx = lax.dynamic_index_in_dim(bx, zh, 1, keepdims=False).reshape(n_quad, width_x, rank)
    by = lax.dynamic_slice_in_dim(basis_y, lax.axis_index("x") * width_y, width_y, 0)
    advanced = stencil(field[:, 0], kappa[0], rates, speeds)[:, None]

    partial = call(
        project_kernel,
        in_specs=[WHOLE, WHOLE],
        out_specs=WHOLE,
        out_shape=stored((own, width_y, rank), F32),
        cost_estimate=cost(2 * n_quad * width_x * own * width_y * rank),
        compiler_params=GRANT,
    )(lines, bx)
    piece = own * width_y // n_zh
    arrived = exchanged(partial.reshape(n_zh, piece, rank), "zh")
    mine = call(
        round_kernel,
        in_specs=[WHOLE],
        out_specs=WHOLE,
        out_shape=stored((n_zh, piece, rank), BF16),
        cost_estimate=cost(10**7),
        compiler_params=GRANT,
    )(arrived)
    projected = exchanged(mine, "zh").reshape(own, width_y, rank)

    moments = call(
        functools.partial(moments_kernel, scale_x),
        in_specs=[WHOLE, WHOLE, WHOLE],
        out_specs=WHOLE,
        out_shape=shape((n_col, 2 * own * rank + n_quad * width_x, rank), BF16),
        cost_estimate=cost(4 * n_quad * width_x * own * width_y * rank),
        compiler_params=GRANT,
    )(lines, projected, by)
    mixed = call(
        functools.partial(mix_kernel, scale_y),
        in_specs=[SCALARS, WHOLE, WHOLE],
        out_specs=WHOLE,
        out_shape=shape((n_quad, own * rank + width_x + part_y, rank), BF16),
        cost_estimate=cost(10**8),
        compiler_params=GRANT,
    )(zh.reshape(1), exchanged(moments, "x"), projected)
    core, rows = call(
        spread_kernel,
        in_specs=[WHOLE],
        out_specs=[WHOLE, WHOLE],
        out_shape=[
            shape((n_quad, own * rank, rank), F32),
            stored((n_grp, width_x + part_y, rank), BF16),
        ],
        cost_estimate=cost(10**8),
        compiler_params=GRANT,
    )(exchanged(mixed, QUAD))
    core = core.reshape(species, 1, rank, rank)
    gram_x, gram_y = call(
        last_kernel,
        in_specs=[WHOLE],
        out_specs=[WHOLE, WHOLE],
        out_shape=[shape((width_x, rank), F32), shape((part_y, rank), F32)],
        cost_estimate=cost(10**7),
        compiler_params=GRANT,
    )(exchanged(rows, GRP))
    return (advanced, core, gram_x, gram_y)


def solution(mesh):
    split = Mesh(
        mesh.devices.reshape(4, 2, 2, 6, 2, 4), ("yh", "core", "yl", "zh", "zl", "x")
    )
    block = P(None, GRP, ROW, "x")
    return jax.shard_map(
        on_device,
        mesh=split,
        in_specs=(block, block, P(GRP, ROW, "x"), P(), P(), P(), P()),
        out_specs=(block, P(None, GRP, None, None), P(ROW, None), P(("x", *ROW), None)),
        check_vma=False,
    )
```

```python
import functools
import math

import jax
import jax.numpy as jnp
from jax import lax
from jax.experimental import pallas as pl
from jax.experimental.pallas import tpu as pltpu
from jax.sharding import Mesh
from jax.sharding import PartitionSpec as P


F32 = jnp.float32
BF16 = jnp.bfloat16
GRP = ("yh", "core")
ROW = ("yl", "zh", "zl")
QUAD = ("yl", "zl")
LANES = 128
WHOLE = pl.BlockSpec(memory_space=pltpu.VMEM)
SCALARS = pl.BlockSpec(memory_space=pltpu.SMEM)


def call(kernel, **given):
    def run(*args):
        return pl.pallas_call(kernel, **given)(*args)

    return run


def chain(n):
    return [(i, i + 1) for i in range(n - 1)]


def back(n):
    return [(i + 1, i) for i in range(n - 1)]


def exchanged(value, axes):
    return lax.all_to_all(value, axes, 0, 0, tiled=True)


def stored(dims, kind):
    return pltpu.HBM(dims, kind)


def shape(dims, kind):
    return jax.ShapeDtypeStruct(dims, kind)


def dot_t(a, b):
    return lax.dot_general(a, b, (((0,), (0,)), ((), ())), preferred_element_type=F32)


def dot(a, b):
    return lax.dot_general(a, b, (((1,), (0,)), ((), ())), preferred_element_type=F32)


GRANT = pltpu.CompilerParams(vmem_limit_bytes=16 * 2**20)


def cost(flops):
    return pl.CostEstimate(flops=flops, bytes_accessed=1 << 20, transcendentals=0)


def faces_kernel(u_ref, low_ref, x_first, x_last, y_first, y_last):
    u = u_ref[0]
    low = u.astype(BF16)
    low_ref[0] = low
    x_first[0] = u[:1]
    x_last[0] = u[-1:]
    y_first[0] = low[:, :LANES]
    y_last[0] = low[:, -LANES:]


def faces(u):
    species, wx, wy = u.shape
    plane = pl.BlockSpec((1, wx, wy), lambda s: (s, 0, 0))
    line = pl.BlockSpec((1, 1, wy), lambda s: (s, 0, 0))
    strip = pl.BlockSpec((1, wx, LANES), lambda s: (s, 0, 0))
    return call(
        faces_kernel,
        grid=(species,),
        in_specs=[plane],
        out_specs=[plane, line, line, strip, strip],
        out_shape=[
            stored(u.shape, BF16),
            stored((species, 1, wy), F32),
            stored((species, 1, wy), F32),
            stored((species, wx, LANES), BF16),
            stored((species, wx, LANES), BF16),
        ],
        cost_estimate=cost(10**8),
        compiler_params=GRANT,
    )(u)


def stencil_kernel(rates, speeds, u_ref, zp, zn, xp, xn, yp, yn, kappa, out):
    s = pl.program_id(0)
    u = u_ref[0]
    wx, wy = u.shape
    rows = lax.broadcasted_iota(jnp.int32, u.shape, 0)
    lanes = lax.broadcasted_iota(jnp.int32, u.shape, 1)
    z_prev, z_next = zp[0].astype(F32), zn[0].astype(F32)
    x_prev = jnp.where(rows == 0, xp[0], pltpu.roll(u, 1, 0))
    x_next = jnp.where(rows == wx - 1, xn[0], pltpu.roll(u, wx - 1, 0))
    y_prev = jnp.where(lanes == 0, yp[0].astype(F32)[:, -1:], pltpu.roll(u, 1, 1))
    y_next = jnp.where(lanes == wy - 1, yn[0].astype(F32)[:, :1], pltpu.roll(u, wy - 1, 1))
    laplace = z_next + z_prev + x_next + x_prev + y_next + y_prev - 6.0 * u
    transport = (
        speeds[s, 0] * (z_next - z_prev)
        + speeds[s, 1] * (x_next - x_prev)
        + speeds[s, 2] * (y_next - y_prev)
    )
    out[0] = u + kappa[...] * rates[s] * laplace - 0.5 * transport


def stencil(u, kappa, rates, speeds):
    species, wx, wy = u.shape
    n_grp, n_row, n_col = lax.axis_size(GRP), lax.axis_size(ROW), lax.axis_size("x")
    low, x_first, x_last, y_first, y_last = faces(u)
    z_prev = lax.ppermute(low, GRP, chain(n_grp))
    z_next = lax.ppermute(low, GRP, back(n_grp))
    x_prev = lax.ppermute(x_last, ROW, chain(n_row))
    x_next = lax.ppermute(x_first, ROW, back(n_row))
    y_prev = lax.ppermute(y_last, "x", chain(n_col))
    y_next = lax.ppermute(y_first, "x", back(n_col))
    plane = pl.BlockSpec((1, wx, wy), lambda s: (s, 0, 0))
    line = pl.BlockSpec((1, 1, wy), lambda s: (s, 0, 0))
    strip = pl.BlockSpec((1, wx, LANES), lambda s: (s, 0, 0))
    return call(
        stencil_kernel,
        grid=(species,),
        in_specs=[SCALARS, SCALARS, plane, plane, plane, line, line, strip, strip]
        + [pl.BlockSpec((wx, wy), lambda s: (0, 0))],
        out_specs=plane,
        out_shape=shape(u.shape, F32),
        cost_estimate=cost(10**9),
        compiler_params=GRANT,
    )(rates, speeds, u, z_prev, z_next, x_prev, x_next, y_prev, y_next, kappa)


def project_kernel(lines, basis, out):
    quad, own, wx, wy = lines.shape
    rank = basis.shape[-1]
    b = basis[...].reshape(quad * wx, rank)
    for s in range(own):
        block = lines[:, s].reshape(quad * wx, wy)
        out[s] = dot_t(block, b)


def round_kernel(parts, out):
    total = parts[0]
    for k in range(1, parts.shape[0]):
        total = total + parts[k]
    low = total.astype(BF16)
    for k in range(out.shape[0]):
        out[k] = low


def moments_kernel(scale, lines, projected, basis, out, rest):
    quad, own, wx, wy = lines.shape
    rank = projected.shape[-1]
    columns = out.shape[0]
    for s in range(own):
        core = dot_t(projected[s], basis[...])
        high = core.astype(BF16)
        rest[pl.ds(s * rank, rank)] = core - high.astype(F32)
        for k in range(columns):
            out[k, pl.ds(s * rank, rank)] = high
    total = dot(lines[:, 0].reshape(quad * wx, wy), projected[0])
    for s in range(1, own):
        total = total + dot(lines[:, s].reshape(quad * wx, wy), projected[s])
    total = (scale * total).astype(BF16)
    for k in range(columns):
        out[k, pl.ds(own * rank, quad * wx)] = total


def mix_kernel(scale, zh, parts, rest, projected, out):
    own, wy, rank = projected.shape
    columns, quad = parts.shape[0], out.shape[0]
    part = (parts.shape[1] - own * rank) // quad
    half_rows = 2 * (out.shape[1] - own * rank - part)
    totals = [0.0, 0.0]
    for s in range(own):
        total = rest[pl.ds(s * rank, rank)]
        for k in range(columns):
            total = total + parts[k, pl.ds(s * rank, rank)].astype(F32)
        low = total.astype(BF16)
        for q in range(quad):
            out[q, pl.ds(s * rank, rank)] = low
        for h in range(2):
            first = pl.multiple_of(h * (wy // 2) + zh[0] * half_rows, half_rows)
            totals[h] = totals[h] + dot(projected[s, pl.ds(first, half_rows), :], low)
    for q in range(quad):
        total = 0.0
        for k in range(columns):
            total = total + parts[k, pl.ds(own * rank + q * part, part)].astype(F32)
        out[q, pl.ds(own * rank, part)] = total.astype(BF16)
    for h in range(2):
        rows = (scale * totals[h]).astype(BF16)
        for low in range(2):
            size = half_rows // 2
            out[2 * h + low, pl.ds(own * rank + part, size)] = rows[low * size : (low + 1) * size]


def spread_kernel(parts, core, out):
    quad, n = parts.shape[0], core.shape[1]
    total = 0.0
    for q in range(quad):
        core[q] = parts[q, :n].astype(F32)
        total = total + parts[q, n:].astype(F32)
    low = total.astype(BF16)
    for k in range(out.shape[0]):
        out[k] = low


def last_kernel(parts, gram_x, gram_y):
    total = parts[0].astype(F32)
    for g in range(1, parts.shape[0]):
        total = total + parts[g].astype(F32)
    n = gram_x.shape[0]
    gram_x[...] = total[:n]
    gram_y[...] = total[n:]


def on_device(field, previous, kappa, rates, speeds, basis_x, basis_y):
    species, depth, width_x, width_y = field.shape
    rank = basis_x.shape[1]
    n_quad, n_zh, n_col = lax.axis_size(QUAD), lax.axis_size("zh"), lax.axis_size("x")
    n_grp, n_row = lax.axis_size(GRP), lax.axis_size(ROW)
    own = species // n_quad
    grid_x, grid_y, grid_z = width_x * n_row, width_y * n_col, depth * n_grp
    part_y = width_y // n_row
    scale_x = math.sqrt(grid_x) / (species * grid_z * grid_y)
    scale_y = math.sqrt(grid_y) / (species * grid_z * rank)
    zh = lax.axis_index("zh")

    lines = exchanged(previous.reshape(n_quad, own, width_x, width_y), QUAD)
    bx = basis_x.reshape(lax.axis_size("yl"), n_zh, lax.axis_size("zl"), width_x, rank)
    bx = lax.dynamic_index_in_dim(bx, zh, 1, keepdims=False).reshape(n_quad, width_x, rank)
    by = lax.dynamic_slice_in_dim(basis_y, lax.axis_index("x") * width_y, width_y, 0)
    advanced = stencil(field[:, 0], kappa[0], rates, speeds)[:, None]

    partial = call(
        project_kernel,
        in_specs=[WHOLE, WHOLE],
        out_specs=WHOLE,
        out_shape=stored((own, width_y, rank), F32),
        cost_estimate=cost(2 * n_quad * width_x * own * width_y * rank),
        compiler_params=GRANT,
    )(lines, bx)
    piece = own * width_y // n_zh
    arrived = exchanged(partial.reshape(n_zh, piece, rank), "zh")
    mine = call(
        round_kernel,
        in_specs=[WHOLE],
        out_specs=WHOLE,
        out_shape=stored((n_zh, piece, rank), BF16),
        cost_estimate=cost(10**7),
        compiler_params=GRANT,
    )(arrived)
    projected = exchanged(mine, "zh").reshape(own, width_y, rank)

    moments, rest = call(
        functools.partial(moments_kernel, scale_x),
        in_specs=[WHOLE, WHOLE, WHOLE],
        out_specs=[WHOLE, WHOLE],
        out_shape=[
            shape((n_col, own * rank + n_quad * width_x, rank), BF16),
            shape((own * rank, rank), F32),
        ],
        cost_estimate=cost(4 * n_quad * width_x * own * width_y * rank),
        compiler_params=GRANT,
    )(lines, projected, by)
    mixed = call(
        functools.partial(mix_kernel, scale_y),
        in_specs=[SCALARS, WHOLE, WHOLE, WHOLE],
        out_specs=WHOLE,
        out_shape=shape((n_quad, own * rank + width_x + part_y, rank), BF16),
        cost_estimate=cost(10**8),
        compiler_params=GRANT,
    )(zh.reshape(1), exchanged(moments, "x"), rest, projected)
    core, rows = call(
        spread_kernel,
        in_specs=[WHOLE],
        out_specs=[WHOLE, WHOLE],
        out_shape=[
            shape((n_quad, own * rank, rank), F32),
            stored((n_grp, width_x + part_y, rank), BF16),
        ],
        cost_estimate=cost(10**8),
        compiler_params=GRANT,
    )(exchanged(mixed, QUAD))
    core = core.reshape(species, 1, rank, rank)
    gram_x, gram_y = call(
        last_kernel,
        in_specs=[WHOLE],
        out_specs=[WHOLE, WHOLE],
        out_shape=[shape((width_x, rank), F32), shape((part_y, rank), F32)],
        cost_estimate=cost(10**7),
        compiler_params=GRANT,
    )(exchanged(rows, GRP))
    return (advanced, core, gram_x, gram_y)


def solution(mesh):
    split = Mesh(
        mesh.devices.reshape(4, 2, 2, 6, 2, 4), ("yh", "core", "yl", "zh", "zl", "x")
    )
    block = P(None, GRP, ROW, "x")
    return jax.shard_map(
        on_device,
        mesh=split,
        in_specs=(block, block, P(GRP, ROW, "x"), P(), P(), P(), P()),
        out_specs=(block, P(None, GRP, None, None), P(ROW, None), P(("x", *ROW), None)),
        check_vma=False,
    )
```
